32 devices in a mesh: grp: 8 (over y, x, core), col: 4 (over z).
Axes of the slice: x: 2, y: 2, z: 4, core: 2. Of those that a mesh axis runs over, the one named last changes fastest.
Arguments:
- old_tables: bfloat16 [32, 128, 32768], P(('grp', 'col')), may hold values from -3 to 3
- table_rows: int32 [32], replicated, may hold values from 4096 to 32768, as said below
- old_plan: int32 [32], replicated, may hold values from 0 to 31, each once
- new_plan: int32 [32], replicated, may hold values from 0 to 31, each once
- ids: int32 [256, 32, 16], P(('grp', 'col')), may hold values from 0 to 32767, as said below
- bag_len: int32 [256, 32], P(('grp', 'col')), may hold values from 1 to 16
Outputs:
- new_tables: bfloat16 [32, 128, 32768], P('grp', 'col')
- pooled: float32 [256, 32, 128], P(('grp', 'col'))
The draws below stay inside these ranges and needn't reach their ends.
Inputs may be any that keep to these rules, and one draw needn't show every extreme that they name: table_rows[t] is a multiple of 4096, and some table has exactly 32768 rows. `ids`: every id of table t lies below table_rows[t].
All inputs are finite; a program needn't handle non-finite values.
Results may differ from the reference program's by a relative error of at most 0.001.
Values may be sent and summed in bfloat16 or wider, within the bound.
No kernel may reach another device: no remote copies, remote signals or barrier semaphores. Data moves between devices by JAX's collectives and lax.ppermute only.
A program may use at most 128 MiB of HBM per device.

```python
import jax
import jax.numpy as jnp
from jax import lax

W = 128
ROWS = 32768
BAG = 16
TABLES = 32
BATCH = 256


def table_sizes(key):
    base = jax.random.fold_in(key, 7)
    eighths = jax.random.randint(jax.random.fold_in(base, 1), (TABLES,), 1, 9)
    chosen = jax.random.randint(jax.random.fold_in(base, 2), (), 0, TABLES)
    eighths = jnp.where(jnp.arange(TABLES) == chosen, 8, eighths)
    return (eighths * (ROWS // 8)).astype(jnp.int32)


def draw_table_rows(key, part):
    return table_sizes(key)


def draw_ids(key, part):
    limits = table_sizes(key)
    drawn = jax.random.randint(jax.random.fold_in(key, 11), (BATCH, TABLES, BAG), 0, limits[None, :, None])
    return drawn.astype(jnp.int32)


def with_ends(values, own_key, low, largest):
    longest = values.shape.index(max(values.shape))
    spots = []
    for shift in (0, 1):
        where = [jax.random.randint(jax.random.fold_in(own_key, axis), (), 0, length) for axis, length in enumerate(values.shape)]
        where[longest] = (where[longest] + shift) % values.shape[longest]
        spots.append(tuple(where))
    return values.at[spots[0]].set(low).at[spots[1]].set(largest)


def shard_levels(key, dims, shards, smallest, largest):
    def one(dim, parts):
        heights = jax.random.uniform(jax.random.fold_in(jax.random.fold_in(key, 6), dim), (parts,), jnp.float32, smallest / len(shards), largest / len(shards))
        return jnp.repeat(jnp.exp(heights), dims[dim] // parts).reshape((-1,) + (1,) * (len(dims) - dim - 1))

    loudness = one(*shards[0])
    for cut in shards[1:]:
        loudness = loudness * one(*cut)
    return loudness


def centred(stream_key, shape, spread, bound, cuts=(), held_as=jnp.bfloat16):
    result = jax.random.normal(stream_key, shape, jnp.float32) * spread
    if len(cuts) > 0:
        result = shard_levels(stream_key, shape, cuts, -0.22, 0.18) * result
    return jnp.clip(result, min=-bound, max=bound).astype(held_as)


def setup_inputs(seed: int = 0) -> dict:
    splits = jax.random.split(jax.random.key(seed), 7)
    return {
        "old_tables": centred(splits[0], (TABLES, W, ROWS), 0.5, 3.0, ((0, 32),)),
        "table_rows": draw_table_rows(jax.random.fold_in(splits[6], 71), 0),
        "old_plan": jax.random.permutation(splits[2], TABLES).astype(jnp.int32),
        "new_plan": jax.random.permutation(splits[3], TABLES).astype(jnp.int32),
        "ids": draw_ids(jax.random.fold_in(splits[6], 71), 0),
        "bag_len": with_ends(jax.random.randint(splits[5], (BATCH, TABLES), 1, BAG + 1), jax.random.fold_in(splits[5], 1), 1, BAG).astype(jnp.int32),
    }


def reference(old_tables, table_rows, old_plan, new_plan, ids, bag_len):
    old_inverse = jnp.argsort(old_plan).astype(jnp.int32)
    new_inverse = jnp.argsort(new_plan).astype(jnp.int32)
    row_iota = jnp.arange(ROWS, dtype=jnp.int32)
    bag_iota = jnp.arange(BAG, dtype=jnp.int32)

    def one_table(position):
        table_id = new_plan[position]
        old_slot = old_inverse[table_id]
        stored = lax.dynamic_index_in_dim(old_tables, old_slot, 0, keepdims=False)
        keep_rows = (row_iota < table_rows[table_id]).astype(old_tables.dtype)
        masked = stored * keep_rows[None, :]
        table_ids = lax.dynamic_index_in_dim(ids, table_id, 1, keepdims=False)
        lengths = lax.dynamic_index_in_dim(bag_len, table_id, 1, keepdims=False)
        values = jnp.take(masked, table_ids, axis=1).astype(jnp.float32)
        in_bag = (bag_iota[None, :] < lengths[:, None]).astype(jnp.float32)
        sums = jnp.sum(values * in_bag[None, :, :], axis=2)
        return masked, sums

    new_tables, sums = lax.map(one_table, jnp.arange(TABLES, dtype=jnp.int32))
    pooled = jnp.transpose(sums[new_inverse], (2, 0, 1))
    return new_tables, pooled
```

```python
import jax
import jax.numpy as jnp
from jax import lax
from jax.experimental import pallas as pl
from jax.experimental.pallas import tpu as pltpu
from jax.sharding import PartitionSpec as P


CHUNKS = 4


def invert(permutation):
    entries = permutation.shape[0]
    across = lax.broadcasted_iota(jnp.int32, (entries, entries), 1)
    down = lax.broadcasted_iota(jnp.int32, (entries, entries), 0)
    return jnp.sum(jnp.where(permutation[None, :] == down, across, 0), axis=1)


def pool_rows(table_cols, marked):
    columns = table_cols.shape[0]
    safe_ids = jnp.maximum(marked, 0).reshape(-1)
    weights = (marked >= 0).astype(jnp.float32)
    picked = (
        jnp.take(table_cols, safe_ids, axis=1)
        .reshape(columns, marked.shape[0], marked.shape[1])
        .astype(jnp.float32)
    )
    return jnp.sum(picked * weights[None, :, :], axis=2)


def split_chunk(table, slot, plan, used_rows, chunk, group_count, col_count):
    full_width, table_len = table.shape
    height = full_width // col_count // CHUNKS
    block = table_len // group_count

    def kernel(slot_ref, plan_ref, used_ref, x_ref, o_ref):
        limit = used_ref[plan_ref[slot_ref[0]]]
        for g in range(group_count):
            rows = lax.broadcasted_iota(jnp.int32, (height, block), 1) + g * block
            piece = x_ref[:, g * block:(g + 1) * block]
            o_ref[g, 0] = jnp.where(rows < limit, piece, jnp.zeros_like(piece))

    return pl.pallas_call(
        kernel,
        grid_spec=pltpu.PrefetchScalarGridSpec(
            num_scalar_prefetch=3,
            grid=(col_count,),
            in_specs=[pl.BlockSpec((height, table_len), lambda c, *_: (c * CHUNKS + chunk, 0))],
            out_specs=pl.BlockSpec((group_count, 1, height, block), lambda c, *_: (0, c, 0, 0)),
        ),
        out_shape=jax.ShapeDtypeStruct((group_count, col_count, height, block), table.dtype),
    )(slot, plan, used_rows, table)


def peer(own, shift, group_count):
    if group_count & (group_count - 1) == 0:
        return own ^ shift
    return (own + shift) % group_count


def peer_pairs(shift, group_count):
    return [(own, peer(own, shift, group_count)) for own in range(group_count)]


def pick_blocks(blocks, source_slot, group_count, per_group):
    _, height, block = blocks.shape

    def kernel(slot_ref, *refs):
        for k in range(group_count):
            refs[group_count + k][...] = refs[k][...]

    def source(k):
        return pl.BlockSpec((1, height, block), lambda p, slots: (slots[k * per_group + p], 0, 0))

    return pl.pallas_call(
        kernel,
        grid_spec=pltpu.PrefetchScalarGridSpec(
            num_scalar_prefetch=1,
            grid=(per_group,),
            in_specs=[source(k) for k in range(group_count)],
            out_specs=[pl.BlockSpec((1, height, block), lambda p, _: (p, 0, 0))] * group_count,
        ),
        out_shape=[jax.ShapeDtypeStruct((per_group, height, block), blocks.dtype)] * group_count,
    )(source_slot, *([blocks] * group_count))


def join_chunk(landed, places, out, chunk):
    group_count = len(landed)
    per_group, height, block = landed[0].shape

    def kernel(place_ref, *refs):
        o_ref = refs[-1]
        for k in range(group_count):
            o_ref[0, :, pl.ds(pl.multiple_of(place_ref[k] * block, block), block)] = refs[k][0]

    shape = jax.ShapeDtypeStruct((per_group, height * CHUNKS, group_count * block), landed[0].dtype)
    first = out is None
    return pl.pallas_call(
        kernel,
        grid_spec=pltpu.PrefetchScalarGridSpec(
            num_scalar_prefetch=1,
            grid=(per_group,),
            in_specs=[pl.BlockSpec((1, height, block), lambda p, _: (p, 0, 0))] * group_count
            + ([] if first else [pl.BlockSpec(memory_space=pl.ANY)]),
            out_specs=pl.BlockSpec((1, height, group_count * block), lambda p, _: (p, chunk, 0)),
        ),
        out_shape=shape,
        input_output_aliases={} if first else {group_count + 1: 0},
    )(places, *landed, *(() if first else (out,)))


def move(old_tables, table_rows, old_plan, new_plan, ids, bag_len):
    group_count = lax.axis_size("grp")
    col_count = lax.axis_size("col")
    device_count = group_count * col_count
    full_width = old_tables.shape[1]
    table_len = old_tables.shape[2]
    row_block = table_len // group_count
    height = full_width // col_count // CHUNKS
    per_group = new_plan.shape[0] // group_count
    bag_size = ids.shape[2]
    own_slot = lax.axis_index("grp") * col_count + lax.axis_index("col")
    slot = own_slot.astype(jnp.int32).reshape(1)
    table = old_tables[0]

    pieces = []
    for k in range(CHUNKS):
        pieces.append(split_chunk(table, slot, old_plan, table_rows, k, group_count, col_count))
    bag_iota = lax.broadcasted_iota(jnp.int32, (1, 1, bag_size), 2)
    marked = jnp.where(bag_iota < bag_len[:, :, None], ids, -1)
    by_slot = jnp.take(marked, old_plan, axis=1)
    own_ids = lax.all_to_all(
        by_slot, ("grp", "col"), split_axis=1, concat_axis=0, tiled=True
    ).reshape(-1, bag_size)
    partial_value = pool_rows(table, own_ids)
    pieces[2], partial_value = lax.optimization_barrier((pieces[2], partial_value))
    old_inverse = invert(old_plan)
    source_slot = old_inverse[new_plan]
    own_group = lax.axis_index("grp").astype(jnp.int32)
    places = peer(own_group, jnp.arange(group_count, dtype=jnp.int32), group_count)
    sources = places
    by_peer = source_slot.reshape(group_count, per_group)[sources].reshape(-1)
    new_local = None
    for k in range(CHUNKS):
        got = lax.all_to_all(
            pieces[k].reshape(device_count, height, row_block),
            ("grp", "col"),
            split_axis=0,
            concat_axis=0,
            tiled=True,
        )
        send = pick_blocks(got, by_peer, group_count, per_group)
        landed = [send[0]] + [
            lax.ppermute(send[shift], "grp", peer_pairs(shift, group_count))
            for shift in range(1, group_count)
        ]
        new_local = join_chunk(landed, places, new_local, k)

    returned = lax.all_to_all(
        partial_value.reshape(1, full_width, -1),
        ("grp", "col"),
        split_axis=2,
        concat_axis=0,
        tiled=True,
    )
    by_table = jnp.take(returned, old_inverse, axis=0)
    pooled = jnp.transpose(by_table, (2, 0, 1))
    return (new_local, pooled)


def solution(mesh):
    return jax.shard_map(
        move,
        mesh=mesh,
        in_specs=(
            P(("grp", "col"), None, None),
            P(),
            P(),
            P(),
            P(("grp", "col"), None, None),
            P(("grp", "col"), None),
        ),
        out_specs=(P("grp", "col", None), P(("grp", "col"), None, None)),
        check_vma=False,
    )
```

```python
import jax
import jax.numpy as jnp
from jax import lax
from jax.experimental import pallas as pl
from jax.experimental.pallas import tpu as pltpu
from jax.sharding import PartitionSpec as P


CHUNKS = 4


def invert(permutation):
    entries = permutation.shape[0]
    across = lax.broadcasted_iota(jnp.int32, (entries, entries), 1)
    down = lax.broadcasted_iota(jnp.int32, (entries, entries), 0)
    return jnp.sum(jnp.where(permutation[None, :] == down, across, 0), axis=1)


def pool_rows(table_rows_first, marks, bag_size):
    safe_ids = jnp.maximum(marks - 1, 0)
    weights = (marks > 0).astype(jnp.float32).reshape(-1, bag_size)
    picked = jnp.take(table_rows_first, safe_ids, axis=0).astype(jnp.float32)
    picked = picked.reshape(-1, bag_size, picked.shape[1])
    return jnp.sum(picked * weights[:, :, None], axis=1)


def write_marks(marks, height, dtype):
    count = marks.shape[0]
    flat = jnp.concatenate([marks >> 8, marks & 255], axis=1).astype(dtype)
    lanes = -(-flat.shape[1] // (height * 128)) * 128
    flat = jnp.pad(flat, ((0, 0), (0, height * lanes - flat.shape[1])))
    return flat.reshape(count, height, lanes)


def read_marks(sent, length):
    flat = sent.reshape(sent.shape[0], -1).astype(jnp.int32)
    return flat[:, :length] * 256 + flat[:, length:2 * length]


def split_chunk(table, slot, plan, used_rows, chunk, group_count, col_count):
    full_width, table_len = table.shape
    height = full_width // col_count // CHUNKS
    block = table_len // group_count

    def kernel(slot_ref, plan_ref, used_ref, x_ref, o_ref):
        limit = used_ref[plan_ref[slot_ref[0]]]
        for g in range(group_count):
            rows = lax.broadcasted_iota(jnp.int32, (height, block), 1) + g * block
            piece = x_ref[:, g * block:(g + 1) * block]
            o_ref[g, 0] = jnp.where(rows < limit, piece, jnp.zeros_like(piece))

    return pl.pallas_call(
        kernel,
        grid_spec=pltpu.PrefetchScalarGridSpec(
            num_scalar_prefetch=3,
            grid=(col_count,),
            in_specs=[pl.BlockSpec((height, table_len), lambda c, *_: (c * CHUNKS + chunk, 0))],
            out_specs=pl.BlockSpec((group_count, 1, height, block), lambda c, *_: (0, c, 0, 0)),
        ),
        out_shape=jax.ShapeDtypeStruct((group_count, col_count, height, block), table.dtype),
    )(slot, plan, used_rows, table)


def peer(own, shift, group_count):
    if group_count & (group_count - 1) == 0:
        return own ^ shift
    return (own + shift) % group_count


def peer_pairs(shift, group_count):
    return [(own, peer(own, shift, group_count)) for own in range(group_count)]


def pick_blocks(blocks, source_slot, group_count, per_group, block):
    height = blocks.shape[1]

    def kernel(slot_ref, *refs):
        for k in range(group_count):
            refs[group_count + k][...] = refs[k][...]

    def source(k):
        return pl.BlockSpec((1, height, block), lambda p, slots: (slots[k * per_group + p], 0, 0))

    return pl.pallas_call(
        kernel,
        grid_spec=pltpu.PrefetchScalarGridSpec(
            num_scalar_prefetch=1,
            grid=(per_group,),
            in_specs=[source(k) for k in range(group_count)],
            out_specs=[pl.BlockSpec((1, height, block), lambda p, _: (p, 0, 0))] * group_count,
        ),
        out_shape=[jax.ShapeDtypeStruct((per_group, height, block), blocks.dtype)] * group_count,
    )(source_slot, *([blocks] * group_count))


def join_chunk(landed, places, out, chunk):
    group_count = len(landed)
    per_group, height, block = landed[0].shape

    def kernel(place_ref, *refs):
        o_ref = refs[-1]
        for k in range(group_count):
            o_ref[0, :, pl.ds(pl.multiple_of(place_ref[k] * block, block), block)] = refs[k][0]

    shape = jax.ShapeDtypeStruct((per_group, height * CHUNKS, group_count * block), landed[0].dtype)
    first = out is None
    return pl.pallas_call(
        kernel,
        grid_spec=pltpu.PrefetchScalarGridSpec(
            num_scalar_prefetch=1,
            grid=(per_group,),
            in_specs=[pl.BlockSpec((1, height, block), lambda p, _: (p, 0, 0))] * group_count
            + ([] if first else [pl.BlockSpec(memory_space=pl.ANY)]),
            out_specs=pl.BlockSpec((1, height, group_count * block), lambda p, _: (p, chunk, 0)),
        ),
        out_shape=shape,
        input_output_aliases={} if first else {group_count + 1: 0},
    )(places, *landed, *(() if first else (out,)))


def move(old_tables, table_rows, old_plan, new_plan, ids, bag_len):
    group_count = lax.axis_size("grp")
    col_count = lax.axis_size("col")
    device_count = group_count * col_count
    full_width = old_tables.shape[1]
    table_len = old_tables.shape[2]
    row_block = table_len // group_count
    height = full_width // col_count // CHUNKS
    per_group = new_plan.shape[0] // group_count
    bag_size = ids.shape[2]
    own_slot = lax.axis_index("grp") * col_count + lax.axis_index("col")
    slot = own_slot.astype(jnp.int32).reshape(1)
    table = old_tables[0]

    pieces = []
    for k in range(CHUNKS):
        pieces.append(split_chunk(table, slot, old_plan, table_rows, k, group_count, col_count))
    bag_iota = lax.broadcasted_iota(jnp.int32, (1, 1, bag_size), 2)
    marked = jnp.where(bag_iota < bag_len[:, :, None], ids + 1, 0)
    own_batch = marked.shape[0]
    by_slot = jnp.transpose(jnp.take(marked, old_plan, axis=1), (1, 0, 2)).reshape(device_count, -1)
    assert table_len <= 65536
    marks_out = write_marks(by_slot, height, table.dtype)
    turned = lax.optimization_barrier(jnp.transpose(table))
    pieces[2], turned = lax.optimization_barrier((pieces[2], turned))
    old_inverse = invert(old_plan)
    source_slot = old_inverse[new_plan]
    own_group = lax.axis_index("grp").astype(jnp.int32)
    places = peer(own_group, jnp.arange(group_count, dtype=jnp.int32), group_count)
    sources = places
    by_peer = source_slot.reshape(group_count, per_group)[sources].reshape(-1)
    new_local = None
    for k in range(CHUNKS):
        leaving = pieces[k].reshape(device_count, height, row_block)
        if k == 1:
            leaving = jnp.concatenate([leaving, marks_out], axis=2)
        got = lax.all_to_all(
            leaving,
            ("grp", "col"),
            split_axis=0,
            concat_axis=0,
            tiled=True,
        )
        if k == 1:
            marks = read_marks(got[:, :, row_block:], own_batch * bag_size).reshape(-1)
            partial_value = pool_rows(turned, marks, bag_size)
            pieces[3], partial_value = lax.optimization_barrier((pieces[3], partial_value))
        send = pick_blocks(got, by_peer, group_count, per_group, row_block)
        landed = [send[0]] + [
            lax.ppermute(send[shift], "grp", peer_pairs(shift, group_count))
            for shift in range(1, group_count)
        ]
        new_local = join_chunk(landed, places, new_local, k)

    returned = lax.all_to_all(
        partial_value.reshape(device_count, own_batch, full_width),
        ("grp", "col"),
        split_axis=0,
        concat_axis=0,
        tiled=True,
    )
    pooled = jnp.transpose(jnp.take(returned, old_inverse, axis=0), (1, 0, 2))
    return (new_local, pooled)


def solution(mesh):
    return jax.shard_map(
        move,
        mesh=mesh,
        in_specs=(
            P(("grp", "col"), None, None),
            P(),
            P(),
            P(),
            P(("grp", "col"), None, None),
            P(("grp", "col"), None),
        ),
        out_specs=(P("grp", "col", None), P(("grp", "col"), None, None)),
        check_vma=False,
    )
```
